32 devices in a mesh: batch: 4 (over z), cols: 8 (over y, x, core).
Axes of the slice: x: 2, y: 2, z: 4, core: 2. Of those that a mesh axis runs over, the one named last changes fastest.
Arguments:
- grad_up: float32 [4, 1024, 4096], P('batch', None, 'cols'), may hold values from -0.875 to 0.875
- grad_down: float32 [4, 4096, 1024], P('batch', 'cols'), may hold values from -0.875 to 0.875
- grad_query: float32 [4, 1024, 1024], P('batch', None, 'cols'), may hold values from -0.875 to 0.875
- grad_key: float32 [4, 1024, 1024], P('batch', None, 'cols'), may hold values from -0.875 to 0.875
- grad_value: float32 [4, 1024, 1024], P('batch', None, 'cols'), may hold values from -0.875 to 0.875
- grad_mixed: float32 [4, 1024, 1024], P('batch', 'cols'), may hold values from -0.875 to 0.875
- grad_norm: float32 [4, 1024], P('batch'), may hold values from -8 to 8
- grad_bias: float32 [4, 1024], P('batch'), may hold values from -8 to 8
- weight_up: float32 [1024, 4096], P('batch', 'cols'), may hold values from -0.25 to 0.25
- weight_down: float32 [4096, 1024], P('cols', 'batch'), may hold values from -0.125 to 0.125
- weight_query: float32 [1024, 1024], P('batch', 'cols'), may hold values from -0.25 to 0.25
- weight_key: float32 [1024, 1024], P('batch', 'cols'), may hold values from -0.25 to 0.25
- weight_value: float32 [1024, 1024], P('batch', 'cols'), may hold values from -0.25 to 0.25
- weight_mixed: float32 [1024, 1024], P('cols', 'batch'), may hold values from -0.25 to 0.25
- weight_norm: float32 [1024], P('batch'), may hold values from 0.25 to 1.75
- weight_bias: float32 [1024], P('batch'), may hold values from -3 to 3
- moment_up: float32 [1024, 4096], P('batch', 'cols'), may hold values from -0.1875 to 0.1875
- moment_down: float32 [4096, 1024], P('cols', 'batch'), may hold values from -0.09375 to 0.09375
- moment_query: float32 [1024, 1024], P('batch', 'cols'), may hold values from -0.1875 to 0.1875
- moment_key: float32 [1024, 1024], P('batch', 'cols'), may hold values from -0.1875 to 0.1875
- moment_value: float32 [1024, 1024], P('batch', 'cols'), may hold values from -0.1875 to 0.1875
- moment_mixed: float32 [1024, 1024], P('cols', 'batch'), may hold values from -0.1875 to 0.1875
- moment_norm: float32 [1024], P('batch'), may hold values from -1.75 to 1.75
- moment_bias: float32 [1024], P('batch'), may hold values from -1.75 to 1.75
Outputs:
- copy_up: bfloat16 [1024, 4096], P(None, 'cols')
- copy_down: bfloat16 [4096, 1024], P('cols')
- copy_query: bfloat16 [1024, 1024], P(None, 'cols')
- copy_key: bfloat16 [1024, 1024], P(None, 'cols')
- copy_value: bfloat16 [1024, 1024], P(None, 'cols')
- copy_mixed: bfloat16 [1024, 1024], P('cols')
- copy_norm: bfloat16 [1024], replicated
- copy_bias: bfloat16 [1024], replicated
- new_up: float32 [1024, 4096], P('batch', 'cols')
- new_down: float32 [4096, 1024], P('cols', 'batch')
- new_query: float32 [1024, 1024], P('batch', 'cols')
- new_key: float32 [1024, 1024], P('batch', 'cols')
- new_value: float32 [1024, 1024], P('batch', 'cols')
- new_mixed: float32 [1024, 1024], P('cols', 'batch')
- new_norm: float32 [1024], P('batch')
- new_bias: float32 [1024], P('batch')
- state_new_up: float32 [1024, 4096], P('batch', 'cols')
- state_new_down: float32 [4096, 1024], P('cols', 'batch')
- state_new_query: float32 [1024, 1024], P('batch', 'cols')
- state_new_key: float32 [1024, 1024], P('batch', 'cols')
- state_new_value: float32 [1024, 1024], P('batch', 'cols')
- state_new_mixed: float32 [1024, 1024], P('cols', 'batch')
- state_new_norm: float32 [1024], P('batch')
- state_new_bias: float32 [1024], P('batch')
The draws below stay inside these ranges and needn't reach their ends.
All inputs are finite; a program needn't handle non-finite values.
Results may differ from the reference program's by a relative error of at most 0.001.
Values may be sent and summed in bfloat16 or wider, within the bound.
No kernel may reach another device: no remote copies, remote signals or barrier semaphores. Data moves between devices by JAX's collectives and lax.ppermute only.
A program may use at most 64 MiB of HBM per device.

```python
import jax
import jax.numpy as jnp
from jax import lax

WIDTH = 1024
INNER = 4096
ATTN = 1024
REPLICAS = 4


def raised(entries, own_key, source, target, shards_of, factor):
    def block_of(axis_at):
        return (jnp.arange(entries.shape[axis_at]) // (entries.shape[axis_at] // shards_of)).reshape((-1,) + (1,) * (entries.ndim - 1 - axis_at))

    one_side = jax.random.permutation(own_key, shards_of)[block_of(target)]
    far = (block_of(target) + shards_of // 2) % shards_of
    return jnp.where((block_of(source) == one_side) | (block_of(source) == far), factor * entries, entries)


def block_scale(stream_key, dims, shards, smallest, largest):
    factor_of = 1.0
    for dim, parts in shards:
        steps = jax.random.uniform(jax.random.fold_in(jax.random.fold_in(stream_key, 6), dim), (parts,), jnp.float32, smallest / len(shards), largest / len(shards))
        factor_of = factor_of * jnp.repeat(jnp.exp(steps), dims[dim] // parts).reshape((-1,) + (1,) * (len(dims) - 1 - dim))
    return factor_of


def centred(rng, shape, width, bound, shards=(), dtype=jnp.bfloat16):
    result = jax.random.normal(rng, shape, jnp.float32) * width
    if len(shards) > 0:
        result = block_scale(rng, shape, shards, -0.22, 0.18) * result
    return jnp.clip(result, min=-bound, max=bound).astype(dtype)


def heavy_noise(stream_key, extent, width, bound, shards, heavy, kind=jnp.bfloat16):
    drawn = width * jax.random.normal(stream_key, extent, jnp.float32)
    if shards:
        drawn = drawn * block_scale(stream_key, extent, shards, -0.22, 0.18)
    return jnp.clip(raised(drawn, jax.random.fold_in(stream_key, 3), *heavy), -bound, bound).astype(kind)


def setup_inputs(seed: int = 0) -> dict:
    splits = jax.random.split(jax.random.key(seed), 25)
    grad_up = heavy_noise(splits[0], (REPLICAS, WIDTH, INNER), 0.1, 0.875, ((0, 4), (2, 8)), (0, 1, 4, 2.0), jnp.float32)
    grad_down = heavy_noise(splits[1], (REPLICAS, INNER, WIDTH), 0.1, 0.875, ((0, 4), (1, 8)), (0, 2, 4, 2.0), jnp.float32)
    grad_query = heavy_noise(splits[2], (REPLICAS, WIDTH, ATTN), 0.1, 0.875, ((0, 4), (2, 8)), (0, 1, 4, 2.0), jnp.float32)
    grad_key = heavy_noise(splits[3], (REPLICAS, WIDTH, ATTN), 0.1, 0.875, ((0, 4), (2, 8)), (0, 1, 4, 2.0), jnp.float32)
    grad_value = heavy_noise(splits[4], (REPLICAS, WIDTH, ATTN), 0.1, 0.875, ((0, 4), (2, 8)), (0, 1, 4, 2.0), jnp.float32)
    grad_mixed = heavy_noise(splits[5], (REPLICAS, ATTN, WIDTH), 0.1, 0.875, ((0, 4), (1, 8)), (0, 2, 4, 2.0), jnp.float32)
    grad_norm = heavy_noise(splits[6], (REPLICAS, WIDTH), 1.0, 8.0, ((0, 4),), (0, 1, 4, 2.0), jnp.float32)
    grad_bias = heavy_noise(splits[7], (REPLICAS, WIDTH), 1.0, 8.0, ((0, 4),), (0, 1, 4, 2.0), jnp.float32)
    weight_up = heavy_noise(splits[8], (WIDTH, INNER), WIDTH ** -0.5, 0.25, ((0, 4), (1, 8)), (1, 0, 8, 2.0), jnp.float32)
    weight_down = heavy_noise(splits[9], (INNER, WIDTH), INNER ** -0.5, 0.125, ((0, 8), (1, 4)), (0, 1, 8, 2.0), jnp.float32)
    weight_query = heavy_noise(splits[10], (WIDTH, ATTN), WIDTH ** -0.5, 0.25, ((0, 4), (1, 8)), (1, 0, 8, 2.0), jnp.float32)
    weight_key = heavy_noise(splits[11], (WIDTH, ATTN), WIDTH ** -0.5, 0.25, ((0, 4), (1, 8)), (1, 0, 8, 2.0), jnp.float32)
    weight_value = heavy_noise(splits[12], (WIDTH, ATTN), WIDTH ** -0.5, 0.25, ((0, 4), (1, 8)), (1, 0, 8, 2.0), jnp.float32)
    weight_mixed = heavy_noise(splits[13], (ATTN, WIDTH), ATTN ** -0.5, 0.25, ((0, 8), (1, 4)), (0, 1, 8, 2.0), jnp.float32)
    weight_norm = jnp.clip(1.0 + 0.15 * jax.random.normal(splits[14], (WIDTH,), jnp.float32), 0.25, 1.75)
    weight_bias = centred(splits[15], (WIDTH,), 0.5, 3.0, ((0, 4),), jnp.float32)
    moment_up = centred(splits[16], (WIDTH, INNER), WIDTH ** -0.5, 0.1875, ((0, 4), (1, 8)), jnp.float32)
    moment_down = centred(splits[17], (INNER, WIDTH), INNER ** -0.5, 0.09375, ((0, 8), (1, 4)), jnp.float32)
    moment_query = centred(splits[18], (WIDTH, ATTN), WIDTH ** -0.5, 0.1875, ((0, 4), (1, 8)), jnp.float32)
    moment_key = centred(splits[19], (WIDTH, ATTN), WIDTH ** -0.5, 0.1875, ((0, 4), (1, 8)), jnp.float32)
    moment_value = centred(splits[20], (WIDTH, ATTN), WIDTH ** -0.5, 0.1875, ((0, 4), (1, 8)), jnp.float32)
    moment_mixed = centred(splits[21], (ATTN, WIDTH), ATTN ** -0.5, 0.1875, ((0, 8), (1, 4)), jnp.float32)
    moment_norm = centred(splits[22], (WIDTH,), 0.3, 1.75, ((0, 4),), jnp.float32)
    moment_bias = centred(splits[23], (WIDTH,), 0.3, 1.75, ((0, 4),), jnp.float32)
    return dict(grad_up=grad_up, grad_down=grad_down, grad_query=grad_query, grad_key=grad_key, grad_value=grad_value, grad_mixed=grad_mixed, grad_norm=grad_norm, grad_bias=grad_bias, weight_up=weight_up, weight_down=weight_down, weight_query=weight_query, weight_key=weight_key, weight_value=weight_value, weight_mixed=weight_mixed, weight_norm=weight_norm, weight_bias=weight_bias, moment_up=moment_up, moment_down=moment_down, moment_query=moment_query, moment_key=moment_key, moment_value=moment_value, moment_mixed=moment_mixed, moment_norm=moment_norm, moment_bias=moment_bias)


learn_rate = 0.4
hold_rate = 0.9

def reference(grad_up, grad_down, grad_query, grad_key, grad_value, grad_mixed, grad_norm, grad_bias, weight_up, weight_down, weight_query, weight_key, weight_value, weight_mixed, weight_norm, weight_bias, moment_up, moment_down, moment_query, moment_key, moment_value, moment_mixed, moment_norm, moment_bias):
    mean_up = lax.optimization_barrier(jnp.sum(grad_up.astype(jnp.float32), axis=0)) * REPLICAS ** (-0.5)
    mean_down = lax.optimization_barrier(jnp.sum(grad_down.astype(jnp.float32), axis=0)) * REPLICAS ** (-0.5)
    mean_query = lax.optimization_barrier(jnp.sum(grad_query.astype(jnp.float32), axis=0)) * REPLICAS ** (-0.5)
    mean_key = lax.optimization_barrier(jnp.sum(grad_key.astype(jnp.float32), axis=0)) * REPLICAS ** (-0.5)
    mean_value = lax.optimization_barrier(jnp.sum(grad_value.astype(jnp.float32), axis=0)) * REPLICAS ** (-0.5)
    mean_mixed = lax.optimization_barrier(jnp.sum(grad_mixed.astype(jnp.float32), axis=0)) * REPLICAS ** (-0.5)
    mean_norm = lax.optimization_barrier(jnp.sum(grad_norm.astype(jnp.float32), axis=0)) * REPLICAS ** (-0.5)
    mean_bias = lax.optimization_barrier(jnp.sum(grad_bias.astype(jnp.float32), axis=0)) * REPLICAS ** (-0.5)
    ratio_up = jnp.sqrt(lax.optimization_barrier(jnp.sum(weight_up * weight_up, axis=1, keepdims=True))) * lax.rsqrt(lax.optimization_barrier(jnp.sum(mean_up * mean_up, axis=1, keepdims=True)) + 1e-06)
    mean_up = mean_up * ratio_up
    ratio_down = jnp.sqrt(lax.optimization_barrier(jnp.sum(weight_down * weight_down, axis=0, keepdims=True))) * lax.rsqrt(lax.optimization_barrier(jnp.sum(mean_down * mean_down, axis=0, keepdims=True)) + 1e-06)
    mean_down = mean_down * ratio_down
    ratio_query = jnp.sqrt(lax.optimization_barrier(jnp.sum(weight_query * weight_query, axis=1, keepdims=True))) * lax.rsqrt(lax.optimization_barrier(jnp.sum(mean_query * mean_query, axis=1, keepdims=True)) + 1e-06)
    mean_query = mean_query * ratio_query
    ratio_key = jnp.sqrt(lax.optimization_barrier(jnp.sum(weight_key * weight_key, axis=1, keepdims=True))) * lax.rsqrt(lax.optimization_barrier(jnp.sum(mean_key * mean_key, axis=1, keepdims=True)) + 1e-06)
    mean_key = mean_key * ratio_key
    ratio_value = jnp.sqrt(lax.optimization_barrier(jnp.sum(weight_value * weight_value, axis=1, keepdims=True))) * lax.rsqrt(lax.optimization_barrier(jnp.sum(mean_value * mean_value, axis=1, keepdims=True)) + 1e-06)
    mean_value = mean_value * ratio_value
    ratio_mixed = jnp.sqrt(lax.optimization_barrier(jnp.sum(weight_mixed * weight_mixed, axis=0, keepdims=True))) * lax.rsqrt(lax.optimization_barrier(jnp.sum(mean_mixed * mean_mixed, axis=0, keepdims=True)) + 1e-06)
    mean_mixed = mean_mixed * ratio_mixed
    state_new_up = hold_rate * moment_up + mean_up
    new_up = weight_up - learn_rate * state_new_up
    state_new_down = hold_rate * moment_down + mean_down
    new_down = weight_down - learn_rate * state_new_down
    state_new_query = hold_rate * moment_query + mean_query
    new_query = weight_query - learn_rate * state_new_query
    state_new_key = hold_rate * moment_key + mean_key
    new_key = weight_key - learn_rate * state_new_key
    state_new_value = hold_rate * moment_value + mean_value
    new_value = weight_value - learn_rate * state_new_value
    state_new_mixed = hold_rate * moment_mixed + mean_mixed
    new_mixed = weight_mixed - learn_rate * state_new_mixed
    state_new_norm = hold_rate * moment_norm + mean_norm
    new_norm = weight_norm - learn_rate * state_new_norm
    state_new_bias = hold_rate * moment_bias + mean_bias
    new_bias = weight_bias - learn_rate * state_new_bias
    copy_up = new_up.astype(jnp.bfloat16)
    copy_down = new_down.astype(jnp.bfloat16)
    copy_query = new_query.astype(jnp.bfloat16)
    copy_key = new_key.astype(jnp.bfloat16)
    copy_value = new_value.astype(jnp.bfloat16)
    copy_mixed = new_mixed.astype(jnp.bfloat16)
    copy_norm = new_norm.astype(jnp.bfloat16)
    copy_bias = new_bias.astype(jnp.bfloat16)
    return (copy_up, copy_down, copy_query, copy_key, copy_value, copy_mixed, copy_norm, copy_bias, new_up, new_down, new_query, new_key, new_value, new_mixed, new_norm, new_bias, state_new_up, state_new_down, state_new_query, state_new_key, state_new_value, state_new_mixed, state_new_norm, state_new_bias)
```

```python
import math

import jax
import jax.numpy as jnp
from jax import lax
from jax.sharding import PartitionSpec as P

learn_rate = 0.4
hold_rate = 0.9

NAMES = ("up", "down", "query", "key", "value", "mixed")
COLUMN_SLICED = ("down", "mixed")
LARGEST_GRAD = 0.875
LARGEST_HALF = 65504.0

CHUNKS = (
    (("query", 0, 1), ("key", 0, 1), ("value", 0, 1), ("up", 0, 1)),
    (("down", 0, 1), ("mixed", 0, 1)),
)


def axis_of(name):
    return 1 if name in COLUMN_SLICED else 0


def pack(pieces, axis):
    return pieces[0] if len(pieces) == 1 else jnp.concatenate(pieces, axis=axis)


def unpack(packed, sizes, axis):
    found, at = [], 0
    for size in sizes:
        found.append(lax.slice_in_dim(packed, at, at + size, axis=axis))
        at += size
    return found


def reduce_line(own_for, n, me):
    scale = 2.0 ** math.floor(math.log2(LARGEST_HALF / (LARGEST_GRAD * n)))
    low = me < n // 2
    right, left = None, None

    def joined(came, term):
        term = term * scale
        return (term if came is None else came.astype(jnp.float32) + term).astype(jnp.float16)

    for step in range(n - 1):
        far = n - 1 - step
        up_pairs = [(i, i + 1) for i in range(n - far)]
        down_pairs = [(i, i - 1) for i in range(far, n)]
        if 2 * step < n - 3:
            came = None if right is None else jnp.where(low, right, left)
            dest = jnp.where(low, jnp.minimum(me + far, n - 1), jnp.maximum(me - far, 0))
            came = lax.ppermute(joined(came, own_for(dest)), "batch", up_pairs + down_pairs)
            none = jnp.zeros_like(came)
            right, left = jnp.where(low, came, none), jnp.where(low, none, came)
        else:
            ahead = joined(right, own_for(jnp.minimum(me + far, n - 1)))
            back = joined(left, own_for(jnp.maximum(me - far, 0)))
            right = lax.ppermute(ahead, "batch", up_pairs)
            left = lax.ppermute(back, "batch", down_pairs)
    total = right.astype(jnp.float32) + left.astype(jnp.float32)
    return own_for(me) + total * (1.0 / scale)


def spread_line(block, n, me):
    right, left = [], []
    ahead, back = block, block
    low = me < n // 2
    for step in range(n - 1):
        up_pairs = [(i, i + 1) for i in range(step, n - 1)]
        down_pairs = [(i, i - 1) for i in range(1, n - step)]
        if n - 1 - step < n // 2:
            came = lax.ppermute(jnp.where(low, back, ahead), "batch", up_pairs + down_pairs)
            ahead, back = came, came
        else:
            ahead = lax.ppermute(ahead, "batch", up_pairs)
            back = lax.ppermute(back, "batch", down_pairs)
        right.append(ahead)
        left.append(back)
    found = [(me, block)]
    for step in range(n - 1):
        found.append(
            (
                lax.rem(me + n - 1 - step, n),
                jnp.where(step < me, right[step], left[n - 2 - step]),
            )
        )
    return found


def reduce_pairs(own_for, n, me):
    scale = 2.0 ** math.floor(math.log2(LARGEST_HALF / (LARGEST_GRAD * n)))
    half = lambda x: x.astype(jnp.float16)
    wide = lambda x: x.astype(jnp.float32)
    came = {}
    step = 1
    while step < n:
        pairs = [(i, i ^ step) for i in range(n)]
        fresh = {}
        for flip in reversed(range(0, n, 2 * step)):
            term = own_for(me ^ step ^ flip) * scale
            for earlier in came:
                if earlier[1] == (flip | step):
                    term = term + wide(came[earlier])
            fresh[(step, flip)] = lax.ppermute(half(term), "batch", pairs)
        came.update(fresh)
        step *= 2
    total = sum(wide(v) for k, v in came.items() if k[1] == 0)
    return own_for(me) + total * (1.0 / scale)


def spread_pairs(block, n, me):
    found = {0: block}
    step = n // 2
    while step:
        pairs = [(i, i ^ step) for i in range(n)]
        for flip, piece in list(found.items()):
            found[flip ^ step] = lax.ppermute(piece, "batch", pairs)
        step //= 2
    return [(me ^ flip, piece) for flip, piece in found.items()]


def sum_cols(values):
    size = lax.axis_size("cols")
    if size & (size - 1):
        return lax.psum(values, "cols")
    step = 1
    while step < size:
        values = values + lax.ppermute(values, "cols", [(i, i ^ step) for i in range(size)])
        step *= 2
    return values


def vectors(grads, weights, moments, n, me):
    width = weights[0].shape[0]
    grads = jnp.stack([g[0] for g in grads])
    parts = jnp.stack([*weights, *moments])
    if n & (n - 1):
        grads = lax.psum(grads, "batch")
        parts = lax.all_gather(parts, "batch", axis=1, tiled=True)
    else:
        step = 1
        while step < n:
            pairs = [(i, i ^ step) for i in range(n)]
            both = lax.ppermute(jnp.concatenate([grads, parts.reshape(2, -1)], axis=1), "batch", pairs)
            cut = grads.shape[1]
            grads = grads + both[:, :cut]
            other = both[:, cut:].reshape(parts.shape)
            low = (me // step) % 2 == 0
            parts = jnp.concatenate(
                [jnp.where(low, parts, other), jnp.where(low, other, parts)], axis=1
            )
            step *= 2
    mean = grads * n ** (-0.5)
    state = hold_rate * parts[2:] + mean
    new = parts[:2] - learn_rate * state
    copies = new.astype(jnp.bfloat16)
    own = lambda x, i: lax.dynamic_slice_in_dim(x[i], me * width, width)
    return (
        [copies[i] for i in range(2)],
        [own(new, i) for i in range(2)],
        [own(state, i) for i in range(2)],
    )


REDUCE, SPREAD = reduce_pairs, spread_pairs


def local(*args):
    grads, weights, moments = args[:8], args[8:16], args[16:24]
    n, me = lax.axis_size("batch"), lax.axis_index("batch")
    rate = n ** (-0.5)
    vec_copy, vec_new, vec_state = vectors(grads[6:], weights[6:], moments[6:], n, me)
    grad = {k: g[0] for k, g in zip(NAMES, grads)}
    weight = dict(zip(NAMES, weights))
    moment = dict(zip(NAMES, moments))

    def sizes(values, name):
        return jnp.sum(values * values, axis=1 - axis_of(name))

    def part_of(array, name, part, parts):
        dim = axis_of(name)
        long = array.shape[dim] // parts
        return lax.slice_in_dim(array, part * long, (part + 1) * long, axis=dim)

    pieces = [p for chunk in CHUNKS for p in chunk]
    lengths = [weight[name].shape[axis_of(name)] // parts for name, part, parts in pieces]
    owns = sum_cols(
        jnp.concatenate([sizes(part_of(weight[p[0]], *p), p[0]) for p in pieces])
    )
    own, at = {}, 0
    for p, long in zip(pieces, lengths):
        own[p] = owns[at : at + long]
        at += long

    states, news, copies = {}, {}, {}
    for chunk in CHUNKS:
        dim = axis_of(chunk[0][0])
        widths = [weight[p[0]].shape[1 - dim] for p in chunk]

        def own_for(dest):
            terms = []
            for name, part, parts in chunk:
                long = weight[name].shape[dim]
                cut = long // parts
                terms.append(
                    lax.dynamic_slice_in_dim(grad[name], dest * long + part * cut, cut, axis=dim)
                )
            return pack(terms, 1 - dim)

        means = unpack(REDUCE(own_for, n, me) * rate, widths, 1 - dim)
        slopes = sum_cols(jnp.concatenate([sizes(m, p[0]) for m, p in zip(means, chunk)]))
        at = 0
        fresh = []
        for mean, p in zip(means, chunk):
            name = p[0]
            long = mean.shape[dim]
            ratio = jnp.sqrt(own[p]) * lax.rsqrt(slopes[at : at + long] + 1e-06)
            at += long
            mean = mean * jnp.expand_dims(ratio, 1 - dim)
            states[p] = hold_rate * part_of(moment[name], *p) + mean
            news[p] = part_of(weight[name], *p) - learn_rate * states[p]
            fresh.append(news[p].astype(jnp.bfloat16))
        for place, block in SPREAD(pack(fresh, 1 - dim), n, me):
            for block, (name, part, parts) in zip(unpack(block, widths, 1 - dim), chunk):
                if name not in copies:
                    copies[name] = jnp.zeros(grad[name].shape, jnp.bfloat16)
                long = weight[name].shape[dim]
                copies[name] = lax.dynamic_update_slice_in_dim(
                    copies[name], block, place * long + part * (long // parts), axis=dim
                )

    def whole(found, name):
        parts = [found[p] for p in pieces if p[0] == name]
        return parts[0] if len(parts) == 1 else jnp.concatenate(parts, axis=axis_of(name))

    return (
        *(copies[k] for k in NAMES),
        *vec_copy,
        *(whole(news, k) for k in NAMES),
        *vec_new,
        *(whole(states, k) for k in NAMES),
        *vec_state,
    )


def solution(mesh):
    row, column = ("batch", "cols"), ("cols", "batch")
    kept = tuple(P(*(column if k in COLUMN_SLICED else row)) for k in NAMES) + (P("batch"),) * 2
    drawn = tuple(
        P("batch", "cols", None) if k in COLUMN_SLICED else P("batch", None, "cols")
        for k in NAMES
    ) + (P("batch", None),) * 2
    copied = tuple(
        P("cols", None) if k in COLUMN_SLICED else P(None, "cols") for k in NAMES
    ) + (P(),) * 2
    return jax.shard_map(
        local,
        mesh=mesh,
        in_specs=drawn + kept + kept,
        out_specs=copied + kept + kept,
        check_vma=False,
    )
```
